32 devices in a mesh: dp: 2 (over core), mp: 16 (over z, y, x).
Axes of the slice: x: 2, y: 2, z: 4, core: 2. Of those that a mesh axis runs over, the one named last changes fastest.
Arguments:
- tokens: bfloat16 [512, 2048], P('dp', 'mp'), may hold values from -6 to 6
- gate_weights: bfloat16 [2, 2048, 7168], P(None, None, 'mp'), may hold values from -0.125 to 0.125
- up_weights: bfloat16 [2, 2048, 7168], P(None, None, 'mp'), may hold values from -0.125 to 0.125
- down_weights: bfloat16 [2, 7168, 2048], P(None, 'mp'), may hold values from -0.0625 to 0.0625
- rhs_gate: float32 [2, 2048, 7168], P(None, 'dp', 'mp'), may hold values from -6 to 6
- rhs_up: float32 [2, 2048, 7168], P(None, 'dp', 'mp'), may hold values from -6 to 6
- rhs_down: float32 [2, 7168, 2048], P(None, 'mp', 'dp'), may hold values from -6 to 6
- damping: float32 [1], replicated, may hold values from 0.5 to 2
Outputs:
- step_gate: float32 [2, 2048, 7168], P(None, 'dp', 'mp')
- step_up: float32 [2, 2048, 7168], P(None, 'dp', 'mp')
- step_down: float32 [2, 7168, 2048], P(None, 'mp', 'dp')
- next_gate: float32 [2, 2048, 7168], P(None, 'dp', 'mp')
- next_up: float32 [2, 2048, 7168], P(None, 'dp', 'mp')
- next_down: float32 [2, 7168, 2048], P(None, 'mp', 'dp')
The draws below stay inside these ranges and needn't reach their ends.
All inputs are finite; a program needn't handle non-finite values.
Results may differ from the reference program's by a relative error of at most 0.007.
Values may be sent and summed in bfloat16 or wider, within the bound.
A program may use at most 128 MiB of HBM per device.

```python
import math
import jax
import jax.numpy as jnp
from jax import lax

D = 2048
FF = 7168
LAYERS = 2
ITERS = 1
TOKENS = 512


def with_spikes(array, rng, source, target, parts, factor):
    def block_of(position):
        return (jnp.arange(array.shape[position]) // (array.shape[position] // parts)).reshape((-1,) + (1,) * (array.ndim - 1 - position))

    near = jax.random.permutation(rng, parts)[block_of(target)]
    far = (block_of(target) + parts // 2) % parts
    return jnp.where((block_of(source) == near) | (block_of(source) == far), factor * array, array)


def steps_of(own_key, shape, cuts, smallest, top_value):
    def one(position, blocks):
        draws = jax.random.uniform(jax.random.fold_in(jax.random.fold_in(own_key, 6), position), (blocks,), jnp.float32, smallest / len(cuts), top_value / len(cuts))
        return jnp.repeat(jnp.exp(draws), shape[position] // blocks).reshape((-1,) + (1,) * (len(shape) - position - 1))

    level = one(*cuts[0])
    for cut in cuts[1:]:
        level = level * one(*cut)
    return level


def bell_draw(stream_key, shape, spread, limit, shards=(), dtype=jnp.bfloat16):
    entries = spread * jax.random.normal(stream_key, shape, jnp.float32)
    if shards:
        entries = entries * steps_of(stream_key, shape, shards, -0.22, 0.18)
    return jnp.clip(entries, -limit, limit).astype(dtype)


def gaussian_with(stream_key, dims, width, limit, split, heavy, held_as=jnp.bfloat16):
    array = width * jax.random.normal(stream_key, dims, jnp.float32)
    if split:
        array = array * steps_of(stream_key, dims, split, -0.22, 0.18)
    return jnp.clip(with_spikes(array, jax.random.fold_in(stream_key, 3), *heavy), -limit, limit).astype(held_as)


def setup_inputs(seed: int = 0) -> dict:
    key_of = jax.random.split(jax.random.key(seed), 9)
    tokens = bell_draw(key_of[0], (TOKENS, D), 1.0, 6.0, ((0, 2), (1, 16)))
    gate_weights = bell_draw(key_of[1], (LAYERS, D, FF), D ** -0.5, 0.125, ((2, 16),))
    up_weights = bell_draw(key_of[2], (LAYERS, D, FF), D ** -0.5, 0.125, ((2, 16),))
    down_weights = bell_draw(key_of[3], (LAYERS, FF, D), FF ** -0.5, 0.0625, ((1, 16),))
    rhs_gate = gaussian_with(key_of[4], (LAYERS, D, FF), 1.0, 6.0, ((1, 2), (2, 16)), (1, 2, 16, 2.0), jnp.float32)
    rhs_up = bell_draw(key_of[5], (LAYERS, D, FF), 1.0, 6.0, ((1, 2), (2, 16)), jnp.float32)
    rhs_down = gaussian_with(key_of[6], (LAYERS, FF, D), 1.0, 6.0, ((1, 16), (2, 2)), (1, 2, 16, 2.0), jnp.float32)
    damping = jnp.clip(jnp.exp(jax.random.uniform(key_of[7], (1,), jnp.float32, math.log(0.5), math.log(2.0))), 0.5, 2.0)
    return dict(tokens=tokens, gate_weights=gate_weights, up_weights=up_weights, down_weights=down_weights, rhs_gate=rhs_gate, rhs_up=rhs_up, rhs_down=rhs_down, damping=damping)


def silu_terms(value):
    sigmoid_value = jax.nn.sigmoid(value)
    return value * sigmoid_value, sigmoid_value * (1.0 + value * (1.0 - sigmoid_value))


def matmul(left, right):
    return jnp.dot(left, right, preferred_element_type=jnp.float32)


def rows_product(left, right):
    return lax.dot_general(left, right, (((0,), (0,)), ((), ())), preferred_element_type=jnp.float32)


def against(left, right):
    return lax.dot_general(left, right, (((1,), (1,)), ((), ())), preferred_element_type=jnp.float32)


def inner(first, second):
    return jnp.sum(first[0] * second[0]) + jnp.sum(first[1] * second[1]) + jnp.sum(first[2] * second[2])


def reference(tokens, gate_weights, up_weights, down_weights, rhs_gate, rhs_up, rhs_down, damping):
    gate_one = matmul(tokens, gate_weights[0])
    up_one = matmul(tokens, up_weights[0])
    active_one, slope_one = silu_terms(gate_one)
    hidden_one = (active_one * up_one).astype(jnp.bfloat16)
    layer_one = (tokens.astype(jnp.float32) + matmul(hidden_one, down_weights[0])).astype(jnp.bfloat16)
    gate_two = matmul(layer_one, gate_weights[1])
    up_two = matmul(layer_one, up_weights[1])
    active_two, slope_two = silu_terms(gate_two)
    hidden_two = (active_two * up_two).astype(jnp.bfloat16)

    def curvature(vectors):
        tangent_gate = vectors[0].astype(jnp.bfloat16)
        tangent_up = vectors[1].astype(jnp.bfloat16)
        tangent_down = vectors[2].astype(jnp.bfloat16)
        tan_gate = matmul(tokens, tangent_gate[0])
        tan_up = matmul(tokens, tangent_up[0])
        tan_hidden = (slope_one * up_one * tan_gate + active_one * tan_up).astype(jnp.bfloat16)
        tan_layer = (matmul(tan_hidden, down_weights[0]) + matmul(hidden_one, tangent_down[0])).astype(jnp.bfloat16)
        tan_gate = matmul(tan_layer, gate_weights[1]) + matmul(layer_one, tangent_gate[1])
        tan_up = matmul(tan_layer, up_weights[1]) + matmul(layer_one, tangent_up[1])
        tan_hidden = (slope_two * up_two * tan_gate + active_two * tan_up).astype(jnp.bfloat16)
        cotan = (tan_layer.astype(jnp.float32) + matmul(tan_hidden, down_weights[1]) + matmul(hidden_two, tangent_down[1])).astype(jnp.bfloat16)
        grad_down_two = rows_product(hidden_two, cotan)
        back_hidden = against(cotan, down_weights[1])
        back_gate = (back_hidden * up_two * slope_two).astype(jnp.bfloat16)
        back_up = (back_hidden * active_two).astype(jnp.bfloat16)
        grad_gate_two = rows_product(layer_one, back_gate)
        grad_up_two = rows_product(layer_one, back_up)
        back_layer = (cotan.astype(jnp.float32) + against(back_gate, gate_weights[1]) + against(back_up, up_weights[1])).astype(jnp.bfloat16)
        grad_down_one = rows_product(hidden_one, back_layer)
        back_hidden = against(back_layer, down_weights[0])
        back_gate = (back_hidden * up_one * slope_one).astype(jnp.bfloat16)
        back_up = (back_hidden * active_one).astype(jnp.bfloat16)
        grad_gate_one = rows_product(tokens, back_gate)
        grad_up_one = rows_product(tokens, back_up)
        scale = 1.0 / TOKENS
        return (jnp.stack([grad_gate_one, grad_gate_two]) * scale + damping[0] * vectors[0],
                jnp.stack([grad_up_one, grad_up_two]) * scale + damping[0] * vectors[1],
                jnp.stack([grad_down_one, grad_down_two]) * scale + damping[0] * vectors[2])

    residual = (rhs_gate, rhs_up, rhs_down)
    direction = residual
    solution = (jnp.zeros_like(rhs_gate), jnp.zeros_like(rhs_up), jnp.zeros_like(rhs_down))
    norm_now = inner(residual, residual)
    for rounds in range(ITERS):
        image = curvature(direction)
        alpha = norm_now / inner(direction, image)
        solution = tuple(solution[k] + alpha * direction[k] for k in range(3))
        residual = tuple(residual[k] - alpha * image[k] for k in range(3))
        norm_next = inner(residual, residual)
        direction = tuple(residual[k] + (norm_next / norm_now) * direction[k] for k in range(3))
        norm_now = norm_next
    return solution[0], solution[1], solution[2], direction[0], direction[1], direction[2]
```

```python
import functools
import jax
import jax.numpy as jnp
from jax import lax
from jax.experimental import pallas as pl
from jax.experimental.pallas import tpu as pltpu
from jax.sharding import PartitionSpec as P

ITERS = 1
MESH = pl.DeviceIdType.MESH


def split_of(count):
    inner = 1
    while inner * inner < count and count % (inner * 2) == 0:
        inner *= 2
    return count // inner, inner


def greet(peers):
    barrier = pltpu.get_barrier_semaphore()
    for peer in peers:
        pl.semaphore_signal(barrier, inc=1, device_id=peer, device_id_type=MESH)
    pl.semaphore_wait(barrier, len(peers))


def place(outer, inner):
    me = lax.axis_index("mp")
    far, near = lax.div(me, inner), lax.rem(me, inner)

    def along_outer(step):
        return {"mp": lax.rem(far + step, outer) * inner + near}

    def along_inner(step):
        return {"mp": far * inner + lax.rem(near + step, inner)}

    return far, near, along_outer, along_inner


def remote(source, target, send, receive, peer):
    copy = pltpu.make_async_remote_copy(
        src_ref=source, dst_ref=target, send_sem=send, recv_sem=receive,
        device_id=peer, device_id_type=MESH,
    )
    copy.start()
    return copy


def sum_kernel(outer, inner, count, adds, *refs):
    parts = refs[:count]
    extra = dict(zip(adds, refs[count:count + len(adds)]))
    outs = refs[count + len(adds):2 * count + len(adds)]
    near_slots, held, far_slots, s1s, s1r, s2s, s2r, g1s, g1r, g2s, g2r = refs[2 * count + len(adds):]
    far, near, along_outer, along_inner = place(outer, inner)
    greet([along_outer(e) for e in range(1, outer)] + [along_inner(d) for d in range(1, inner)])
    order = list(range(1, outer)) + [0]
    copies = []
    first, second, third, fourth = {}, {}, {}, {}
    for e in order:
        piece = lax.rem(far + e, outer)
        for k in range(count):
            for d in range(1, inner):
                first[k, d, e] = remote(
                    parts[k].at[lax.rem(near + d, inner), piece], near_slots.at[k, d, e],
                    s1s.at[k, d, e], s1r.at[k, d, e], along_inner(d),
                )
    own = {}
    for e in order:
        piece = lax.rem(far + e, outer)
        for k in range(count):
            total = parts[k][near, piece].astype(jnp.float32)
            for d in range(1, inner):
                first[k, d, e].wait_recv()
                total = total + near_slots[k, d, e].astype(jnp.float32)
            if e:
                held[k, e] = total.astype(jnp.bfloat16)
                second[k, e] = remote(
                    held.at[k, e], far_slots.at[k, e], s2s.at[k, e], s2r.at[k, e], along_outer(e)
                )
            else:
                own[k] = total
    for k in range(count):
        total = own[k]
        for e in range(1, outer):
            second[k, e].wait_recv()
            total = total + far_slots[k, e].astype(jnp.float32)
        if k in extra:
            total = total + extra[k][near, far].astype(jnp.float32)
        outs[k][near, far] = total.astype(jnp.bfloat16)
        spread(outer, inner, outs[k], far, near, along_outer, along_inner, third, fourth, k,
               g1s, g1r, g2s, g2r)
    forward(outer, inner, outs, far, near, along_inner, third, fourth, g2s, g2r)
    for table in (first, second, third, fourth):
        for copy in table.values():
            copy.wait_send()


def spread(outer, inner, out, far, near, along_outer, along_inner, third, fourth, k, g1s, g1r, g2s, g2r):
    for e in range(1, outer):
        third[k, e] = remote(out.at[near, far], out.at[near, far], g1s.at[k, e], g1r.at[k, e], along_outer(e))
    for d in range(1, inner):
        fourth[k, d, 0] = remote(
            out.at[near, far], out.at[near, far], g2s.at[k, d, 0], g2r.at[k, d, 0], along_inner(d)
        )


def forward(outer, inner, outs, far, near, along_inner, third, fourth, g2s, g2r):
    for e in range(1, outer):
        piece = lax.rem(far - e + outer, outer)
        for k in range(len(outs)):
            third[k, e].wait_recv()
            for d in range(1, inner):
                fourth[k, d, e] = remote(
                    outs[k].at[near, piece], outs[k].at[near, piece],
                    g2s.at[k, d, e], g2r.at[k, d, e], along_inner(d),
                )
    for copy in fourth.values():
        copy.wait_recv()


def summed_whole(mp, parts, adds, ident):
    outer, inner = split_of(mp)
    rows, width = parts[0].shape
    share = rows // mp
    count = len(parts)
    view = (inner, outer, share, width)
    which = tuple(k for k in range(count) if adds[k] is not None)
    operands = [p.astype(jnp.bfloat16).reshape(view) for p in parts]
    operands += [adds[k].reshape(view) for k in which]
    dma = pltpu.SemaphoreType.DMA
    outs = pl.pallas_call(
        functools.partial(sum_kernel, outer, inner, count, which),
        out_shape=[jax.ShapeDtypeStruct(view, jnp.bfloat16)] * count,
        in_specs=[pl.BlockSpec(memory_space=pltpu.VMEM)] * len(operands),
        out_specs=[pl.BlockSpec(memory_space=pltpu.VMEM)] * count,
        scratch_shapes=[
            pltpu.VMEM((count, inner, outer, share, width), jnp.bfloat16),
            pltpu.VMEM((count, outer, share, width), jnp.bfloat16),
            pltpu.VMEM((count, outer, share, width), jnp.bfloat16),
            dma((count, inner, outer)), dma((count, inner, outer)),
            dma((count, outer)), dma((count, outer)),
            dma((count, outer)), dma((count, outer)),
            dma((count, inner, outer)), dma((count, inner, outer)),
        ],
        cost_estimate=pl.CostEstimate(
            flops=0, bytes_accessed=count * rows * width * 64, transcendentals=0
        ),
        compiler_params=pltpu.CompilerParams(collective_id=ident, has_side_effects=True),
    )(*operands)
    return [o.reshape(rows, width) for o in outs]


def gather_kernel(outer, inner, mine, out, local, g1s, g1r, g2s, g2r):
    far, near, along_outer, along_inner = place(outer, inner)
    greet([along_outer(e) for e in range(1, outer)] + [along_inner(d) for d in range(1, inner)])
    third, fourth = {}, {}
    keep = pltpu.make_async_copy(mine, out.at[far, near], local)
    keep.start()
    for e in range(1, outer):
        third[e] = remote(mine, out.at[far, near], g1s.at[e], g1r.at[e], along_outer(e))
    for d in range(1, inner):
        fourth[d, 0] = remote(mine, out.at[far, near], g2s.at[d, 0], g2r.at[d, 0], along_inner(d))
    for e in range(1, outer):
        piece = lax.rem(far - e + outer, outer)
        third[e].wait_recv()
        for d in range(1, inner):
            fourth[d, e] = remote(
                out.at[piece, near], out.at[piece, near], g2s.at[d, e], g2r.at[d, e], along_inner(d)
            )
    for copy in fourth.values():
        copy.wait_recv()
    keep.wait()
    for table in (third, fourth):
        for copy in table.values():
            copy.wait_send()


def gathered(mp, tokens, ident):
    outer, inner = split_of(mp)
    rows, share = tokens.shape
    dma = pltpu.SemaphoreType.DMA
    out = pl.pallas_call(
        functools.partial(gather_kernel, outer, inner),
        out_shape=jax.ShapeDtypeStruct((outer, inner, rows, share), tokens.dtype),
        in_specs=[pl.BlockSpec(memory_space=pltpu.VMEM)],
        out_specs=pl.BlockSpec(memory_space=pltpu.VMEM),
        scratch_shapes=[dma, dma((outer,)), dma((outer,)), dma((inner, outer)), dma((inner, outer))],
        cost_estimate=pl.CostEstimate(
            flops=0, bytes_accessed=rows * share * mp * 32, transcendentals=0
        ),
        compiler_params=pltpu.CompilerParams(collective_id=ident, has_side_effects=True),
    )(tokens)
    return out.reshape(mp, rows, share).transpose(1, 0, 2).reshape(rows, mp * share)


def scalar_kernel(dp, mp, mine, out, slots, send, receive):
    row, column = lax.axis_index("dp"), lax.axis_index("mp")
    total = dp * mp
    me = row * mp + column

    def other(step):
        index = lax.rem(me + step, total)
        return {"dp": lax.div(index, mp), "mp": lax.rem(index, mp)}

    greet([other(step) for step in range(1, total)])
    copies = [
        remote(mine, slots.at[me], send.at[step], receive.at[step], other(step))
        for step in range(1, total)
    ]
    slots[me] = mine[...]
    for copy in copies:
        copy.wait_recv()
    out[...] = jnp.sum(slots[...], axis=0)
    for copy in copies:
        copy.wait_send()


def scalars_summed(dp, mp, values, ident):
    packed = jnp.stack(values)
    packed = jnp.pad(packed, (0, 128 - len(values)))
    packed = jnp.broadcast_to(packed[None], (8, 128))
    total = dp * mp
    dma = pltpu.SemaphoreType.DMA
    out = pl.pallas_call(
        functools.partial(scalar_kernel, dp, mp),
        out_shape=jax.ShapeDtypeStruct((8, 128), jnp.float32),
        in_specs=[pl.BlockSpec(memory_space=pltpu.VMEM)],
        out_specs=pl.BlockSpec(memory_space=pltpu.VMEM),
        scratch_shapes=[pltpu.VMEM((total, 8, 128), jnp.float32), dma((total,)), dma((total,))],
        compiler_params=pltpu.CompilerParams(collective_id=ident, has_side_effects=True),
    )(packed)
    return [out[0, k] for k in range(len(values))]


def silu_terms(value):
    sigmoid_value = jax.nn.sigmoid(value)
    return (value * sigmoid_value, sigmoid_value * (1.0 + value * (1.0 - sigmoid_value)))


def matmul(left, right):
    return jnp.dot(left, right, preferred_element_type=jnp.float32)


def rows_product(left, right):
    return lax.dot_general(
        left, right, (((0,), (0,)), ((), ())), preferred_element_type=jnp.float32
    )


def against(left, right):
    return lax.dot_general(
        left, right, (((1,), (1,)), ((), ())), preferred_element_type=jnp.float32
    )


def body(tokens, gate_weights, up_weights, down_weights, rhs_gate, rhs_up, rhs_down, damping):
    dp, mp = lax.axis_size("dp"), lax.axis_size("mp")
    scale = 1.0 / (tokens.shape[0] * dp)
    rhs = (rhs_gate, rhs_up, rhs_down)
    axes = (0, 0, 1)

    def tangents(layer):
        return tuple(
            lax.all_gather(rhs[k][layer].astype(jnp.bfloat16), "dp", axis=axes[k], tiled=True)
            for k in range(3)
        )

    def scattered(grads):
        return tuple(
            lax.psum_scatter(
                grads[k].astype(jnp.bfloat16), "dp", scatter_dimension=axes[k], tiled=True
            ).astype(jnp.float32)
            for k in range(3)
        )

    whole = gathered(mp, tokens, 0)
    tangent_gate, tangent_up, tangent_down = tangents(0)
    next_gate, next_up, next_down = tangents(1)
    gate_one = matmul(whole, gate_weights[0])
    up_one = matmul(whole, up_weights[0])
    active_one, slope_one = silu_terms(gate_one)
    hidden_one = (active_one * up_one).astype(jnp.bfloat16)
    tan_gate = matmul(whole, tangent_gate)
    tan_up = matmul(whole, tangent_up)
    tan_hidden = (slope_one * up_one * tan_gate + active_one * tan_up).astype(jnp.bfloat16)
    layer_one, tan_layer = summed_whole(
        mp,
        (
            matmul(hidden_one, down_weights[0]),
            matmul(tan_hidden, down_weights[0]) + matmul(hidden_one, tangent_down),
        ),
        (whole, None),
        1,
    )
    gate_two = matmul(layer_one, gate_weights[1])
    up_two = matmul(layer_one, up_weights[1])
    active_two, slope_two = silu_terms(gate_two)
    hidden_two = (active_two * up_two).astype(jnp.bfloat16)
    tan_gate = matmul(tan_layer, gate_weights[1]) + matmul(layer_one, next_gate)
    tan_up = matmul(tan_layer, up_weights[1]) + matmul(layer_one, next_up)
    tan_hidden = (slope_two * up_two * tan_gate + active_two * tan_up).astype(jnp.bfloat16)
    (cotan,) = summed_whole(
        mp,
        (matmul(tan_hidden, down_weights[1]) + matmul(hidden_two, next_down),),
        (tan_layer,),
        2,
    )
    back_hidden = against(cotan, down_weights[1])
    back_gate = (back_hidden * up_two * slope_two).astype(jnp.bfloat16)
    back_up = (back_hidden * active_two).astype(jnp.bfloat16)
    (back_layer,) = summed_whole(
        mp,
        (against(back_gate, gate_weights[1]) + against(back_up, up_weights[1]),),
        (cotan,),
        3,
    )
    second = scattered(
        (
            rows_product(layer_one, back_gate),
            rows_product(layer_one, back_up),
            rows_product(hidden_two, cotan),
        )
    )
    back_hidden = against(back_layer, down_weights[0])
    back_gate = (back_hidden * up_one * slope_one).astype(jnp.bfloat16)
    back_up = (back_hidden * active_one).astype(jnp.bfloat16)
    first = scattered(
        (
            rows_product(whole, back_gate),
            rows_product(whole, back_up),
            rows_product(hidden_one, back_layer),
        )
    )
    grads = (first, second)
    norm = crossed = squared = 0.0
    for layer in range(2):
        for k in range(3):
            right, grad = rhs[k][layer], grads[layer][k]
            norm = norm + jnp.sum(right * right)
            crossed = crossed + jnp.sum(right * grad)
            squared = squared + jnp.sum(grad * grad)
    norm, crossed, squared = scalars_summed(dp, mp, (norm, crossed, squared), 4)
    damp = damping[0]
    along = crossed * scale + damp * norm
    image = squared * scale * scale + 2.0 * damp * scale * crossed + damp * damp * norm
    alpha = norm / along
    norm_next = norm - 2.0 * alpha * along + alpha * alpha * image
    beta = norm_next / norm
    steps = tuple(alpha * rhs[k] for k in range(3))
    nexts = tuple(
        jnp.stack(
            [
                rhs[k][layer]
                - alpha * (grads[layer][k] * scale + damp * rhs[k][layer])
                + beta * rhs[k][layer]
                for layer in range(2)
            ]
        )
        for k in range(3)
    )
    return steps + nexts


def solution(mesh):
    in_specs = (
        P("dp", "mp"),
        P(None, None, "mp"),
        P(None, None, "mp"),
        P(None, "mp", None),
        P(None, "dp", "mp"),
        P(None, "dp", "mp"),
        P(None, "mp", "dp"),
        P(),
    )
    out_specs = (
        P(None, "dp", "mp"),
        P(None, "dp", "mp"),
        P(None, "mp", "dp"),
        P(None, "dp", "mp"),
        P(None, "dp", "mp"),
        P(None, "mp", "dp"),
    )
    return jax.shard_map(body, mesh=mesh, in_specs=in_specs, out_specs=out_specs, check_vma=False)
```

```python
import functools
import jax
import jax.numpy as jnp
from jax import lax
from jax.experimental import pallas as pl
from jax.experimental.pallas import tpu as pltpu
from jax.sharding import PartitionSpec as P

ITERS = 1
MESH = pl.DeviceIdType.MESH


def split_of(count):
    inner = 1
    while inner * inner < count and count % (inner * 2) == 0:
        inner *= 2
    return count // inner, inner


def greet(peers):
    barrier = pltpu.get_barrier_semaphore()
    for peer in peers:
        pl.semaphore_signal(barrier, inc=1, device_id=peer, device_id_type=MESH)
    pl.semaphore_wait(barrier, len(peers))


def place(outer, inner):
    me = lax.axis_index("mp")
    far, near = lax.div(me, inner), lax.rem(me, inner)

    def along_outer(step):
        return {"mp": lax.rem(far + step, outer) * inner + near}

    def along_inner(step):
        return {"mp": far * inner + lax.rem(near + step, inner)}

    return far, near, along_outer, along_inner


def remote(source, target, send, receive, peer):
    copy = pltpu.make_async_remote_copy(
        src_ref=source, dst_ref=target, send_sem=send, recv_sem=receive,
        device_id=peer, device_id_type=MESH,
    )
    copy.start()
    return copy


def start_pairs(sources, pairs, send, receive):
    row = lax.axis_index("dp")
    copies = []
    for k, (source, pair) in enumerate(zip(sources, pairs)):
        width = pair.shape[-1]
        if source.shape[-1] == width:
            outgoing = source
        else:
            outgoing = source.at[:, pl.ds(pl.multiple_of((1 - row) * width, width), width)]
        copies.append(remote(outgoing, pair.at[1], send.at[k], receive.at[k], {"dp": 1 - row}))
    return copies


def keep_pairs(sources, pairs):
    row = lax.axis_index("dp")
    for source, pair in zip(sources, pairs):
        width = pair.shape[-1]
        if source.shape[-1] == width:
            pair[0] = source[...]
        else:
            pair[0] = source[:, pl.ds(pl.multiple_of(row * width, width), width)]


def sum_kernel(outer, inner, count, adds, paired, *refs):
    parts = refs[:count]
    extra = dict(zip(adds, refs[count:count + len(adds)]))
    base = count + len(adds)
    sources = refs[base:base + paired]
    base += paired
    outs = refs[base:base + count]
    base += count
    pairs = refs[base:base + paired]
    base += paired
    near_slots, held, far_slots, s1s, s1r, s2s, s2r, g1s, g1r, g2s, g2r = refs[base:base + 11]
    far, near, along_outer, along_inner = place(outer, inner)
    peers = [along_outer(e) for e in range(1, outer)] + [along_inner(d) for d in range(1, inner)]
    if paired:
        peers.append({"dp": 1 - lax.axis_index("dp")})
    greet(peers)
    order = list(range(1, outer)) + [0]
    copies = []
    first, second, third, fourth = {}, {}, {}, {}
    for e in order:
        piece = lax.rem(far + e, outer)
        for k in range(count):
            for d in range(1, inner):
                first[k, d, e] = remote(
                    parts[k].at[lax.rem(near + d, inner), piece], near_slots.at[k, d, e],
                    s1s.at[k, d, e], s1r.at[k, d, e], along_inner(d),
                )
    swaps = start_pairs(sources, pairs, *refs[base + 11:]) if paired else []
    keep_pairs(sources, pairs)
    own = {}
    for e in order:
        piece = lax.rem(far + e, outer)
        for k in range(count):
            total = parts[k][near, piece].astype(jnp.float32)
            for d in range(1, inner):
                first[k, d, e].wait_recv()
                total = total + near_slots[k, d, e].astype(jnp.float32)
            if e:
                held[k, e] = total.astype(jnp.bfloat16)
                second[k, e] = remote(
                    held.at[k, e], far_slots.at[k, e], s2s.at[k, e], s2r.at[k, e], along_outer(e)
                )
            else:
                own[k] = total
    for k in range(count):
        total = own[k]
        for e in range(1, outer):
            second[k, e].wait_recv()
            total = total + far_slots[k, e].astype(jnp.float32)
        if k in extra:
            total = total + extra[k][near, far].astype(jnp.float32)
        outs[k][near, far] = total.astype(jnp.bfloat16)
        spread(outer, inner, outs[k], far, near, along_outer, along_inner, third, fourth, k,
               g1s, g1r, g2s, g2r)
    forward(outer, inner, outs, far, near, along_inner, third, fourth, g2s, g2r)
    for copy in swaps:
        copy.wait()
    for table in (first, second, third, fourth):
        for copy in table.values():
            copy.wait_send()


def spread(outer, inner, out, far, near, along_outer, along_inner, third, fourth, k, g1s, g1r, g2s, g2r):
    for e in range(1, outer):
        third[k, e] = remote(out.at[near, far], out.at[near, far], g1s.at[k, e], g1r.at[k, e], along_outer(e))
    for d in range(1, inner):
        fourth[k, d, 0] = remote(
            out.at[near, far], out.at[near, far], g2s.at[k, d, 0], g2r.at[k, d, 0], along_inner(d)
        )


def forward(outer, inner, outs, far, near, along_inner, third, fourth, g2s, g2r):
    for e in range(1, outer):
        piece = lax.rem(far - e + outer, outer)
        for k in range(len(outs)):
            third[k, e].wait_recv()
            for d in range(1, inner):
                fourth[k, d, e] = remote(
                    outs[k].at[near, piece], outs[k].at[near, piece],
                    g2s.at[k, d, e], g2r.at[k, d, e], along_inner(d),
                )
    for copy in fourth.values():
        copy.wait_recv()


def summed_whole(mp, parts, adds, ident, full=(), half=()):
    outer, inner = split_of(mp)
    rows, width = parts[0].shape
    share = rows // mp
    count = len(parts)
    view = (inner, outer, share, width)
    which = tuple(k for k in range(count) if adds[k] is not None)
    operands = [p.astype(jnp.bfloat16).reshape(view) for p in parts]
    operands += [adds[k].reshape(view) for k in which]
    dma = pltpu.SemaphoreType.DMA
    paired = len(full) + len(half)
    operands += list(full) + list(half)
    outs = pl.pallas_call(
        functools.partial(sum_kernel, outer, inner, count, which, paired),
        out_shape=[jax.ShapeDtypeStruct(view, jnp.bfloat16)] * count + pair_shapes(full, half),
        in_specs=[pl.BlockSpec(memory_space=pltpu.VMEM)] * len(operands),
        out_specs=[pl.BlockSpec(memory_space=pltpu.VMEM)] * (count + paired),
        scratch_shapes=[
            pltpu.VMEM((count, inner, outer, share, width), jnp.bfloat16),
            pltpu.VMEM((count, outer, share, width), jnp.bfloat16),
            pltpu.VMEM((count, outer, share, width), jnp.bfloat16),
            dma((count, inner, outer)), dma((count, inner, outer)),
            dma((count, outer)), dma((count, outer)),
            dma((count, outer)), dma((count, outer)),
            dma((count, inner, outer)), dma((count, inner, outer)),
        ] + [dma((paired,))] * (2 if paired else 0),
        cost_estimate=pl.CostEstimate(
            flops=0, bytes_accessed=count * rows * width * 64, transcendentals=0
        ),
        compiler_params=pltpu.CompilerParams(collective_id=ident, has_side_effects=True),
    )(*operands)
    return [o.reshape(rows, width) for o in outs[:count]] + joined(outs[count:])


def pair_shapes(full, half):
    return [jax.ShapeDtypeStruct((2,) + x.shape, x.dtype) for x in full] + [
        jax.ShapeDtypeStruct((2, x.shape[0], x.shape[1] // 2), x.dtype) for x in half
    ]


def joined(pairs):
    return [p.reshape(2 * p.shape[1], p.shape[2]) for p in pairs]


def pair_kernel(paired, *refs):
    sources, pairs = refs[:paired], refs[paired:2 * paired]
    greet([{"dp": 1 - lax.axis_index("dp")}])
    copies = start_pairs(sources, pairs, *refs[2 * paired:])
    keep_pairs(sources, pairs)
    for copy in copies:
        copy.wait()


def swapped(full, half, ident):
    paired = len(full) + len(half)
    spec = [pl.BlockSpec(memory_space=pltpu.VMEM)] * paired
    dma = pltpu.SemaphoreType.DMA
    return joined(
        pl.pallas_call(
            functools.partial(pair_kernel, paired),
            out_shape=pair_shapes(full, half),
            in_specs=spec,
            out_specs=spec,
            scratch_shapes=[dma((paired,)), dma((paired,))],
            compiler_params=pltpu.CompilerParams(collective_id=ident, has_side_effects=True),
        )(*full, *half)
    )


def chunk_of(rows):
    return next(c for c in (64, 112, 32, 16, 8) if rows % c == 0)


def folded(block):
    return jnp.sum(block.reshape(block.shape[0] // 8, 8, block.shape[1]), axis=0)


def gather_kernel(outer, inner, mine, gate, up, down, out, norm, *refs):
    tangents, scratch = refs[:6], refs[6:]
    held, local, loads, g1s, g1r, g2s, g2r, ts, tr = scratch
    blocks = [(source, layer) for layer in range(2) for source in (gate, up, down)]
    fetches = []
    for k, (source, layer) in enumerate(blocks):
        fetches.append(pltpu.make_async_copy(source.at[layer], held.at[k], loads.at[k]))
        fetches[k].start()
    far, near, along_outer, along_inner = place(outer, inner)
    row = lax.axis_index("dp")
    greet(
        [along_outer(e) for e in range(1, outer)]
        + [along_inner(d) for d in range(1, inner)]
        + [{"dp": 1 - row}]
    )
    third, fourth = {}, {}
    keep = pltpu.make_async_copy(mine, out.at[far, near], local)
    keep.start()
    for e in range(1, outer):
        third[e] = remote(mine, out.at[far, near], g1s.at[e], g1r.at[e], along_outer(e))
    for d in range(1, inner):
        fourth[d, 0] = remote(mine, out.at[far, near], g2s.at[d, 0], g2r.at[d, 0], along_inner(d))
    rows, width = held.shape[1:]
    chunk = chunk_of(rows)
    columns = pl.ds(pl.multiple_of(row * width, width), width)
    total = jnp.zeros((8, width), jnp.float32)
    swaps = []

    def convert(k, total):
        fetches[k].wait()

        def piece(step, carry):
            span = pl.ds(pl.multiple_of(step * chunk, chunk), chunk)
            value = held[k, span]
            tangents[k][span, columns] = value.astype(jnp.bfloat16)
            return carry + folded(value * value)

        total = lax.fori_loop(0, rows // chunk, piece, total)
        swaps.append(
            remote(tangents[k].at[:, columns], tangents[k].at[:, columns], ts.at[k], tr.at[k], {"dp": 1 - row})
        )
        return total

    def relay(e):
        piece = lax.rem(far - e + outer, outer)
        third[e].wait_recv()
        for d in range(1, inner):
            fourth[d, e] = remote(
                out.at[piece, near], out.at[piece, near], g2s.at[d, e], g2r.at[d, e], along_inner(d)
            )

    total = convert(0, total)
    total = convert(1, total)
    for e in range(1, outer):
        relay(e)
    for k in range(2, 6):
        total = convert(k, total)
    norm[...] = total
    for copy in fourth.values():
        copy.wait_recv()
    keep.wait()
    for copy in swaps:
        copy.wait()
    for table in (third, fourth):
        for copy in table.values():
            copy.wait_send()


def gathered(mp, tokens, rhs, ident):
    outer, inner = split_of(mp)
    rows, share = tokens.shape
    hidden, width = rhs[0].shape[1:]
    dma = pltpu.SemaphoreType.DMA
    vmem, anywhere = pl.BlockSpec(memory_space=pltpu.VMEM), pl.BlockSpec(memory_space=pl.ANY)
    out, norm, *tangents = pl.pallas_call(
        functools.partial(gather_kernel, outer, inner),
        out_shape=[
            jax.ShapeDtypeStruct((outer, inner, rows, share), tokens.dtype),
            jax.ShapeDtypeStruct((8, width), jnp.float32),
        ] + [jax.ShapeDtypeStruct((hidden, 2 * width), jnp.bfloat16)] * 6,
        in_specs=[vmem] + [anywhere] * 3,
        out_specs=[vmem] * 8,
        scratch_shapes=[
            pltpu.VMEM((6, hidden, width), jnp.float32),
            dma, dma((6,)), dma((outer,)), dma((outer,)), dma((inner, outer)), dma((inner, outer)),
            dma((6,)), dma((6,)),
        ],
        compiler_params=pltpu.CompilerParams(
            collective_id=ident, has_side_effects=True, vmem_limit_bytes=48 * 1024 * 1024
        ),
    )(tokens, *rhs)
    whole = out.reshape(mp, rows, share).transpose(1, 0, 2).reshape(rows, mp * share)
    return whole, norm, tangents


def scalar_kernel(dp, mp, scale, norm, damping, gate, up, down, *refs):
    grads, (out, right, held, packed, slots, loads, send, receive) = refs[:6], refs[6:]
    row, column = lax.axis_index("dp"), lax.axis_index("mp")
    total = dp * mp
    me = row * mp + column

    def other(step):
        index = lax.rem(me + step, total)
        return {"dp": lax.div(index, mp), "mp": lax.rem(index, mp)}

    barrier = pltpu.get_barrier_semaphore()
    for step in range(1, total):
        pl.semaphore_signal(barrier, inc=1, device_id=other(step), device_id_type=MESH)
    blocks = [(source, layer) for layer in range(2) for source in (gate, up, down)]
    fetches = []
    for k, (source, layer) in enumerate(blocks):
        fetches.append(
            (
                pltpu.make_async_copy(source.at[layer], right.at[k], loads.at[k, 0]),
                pltpu.make_async_copy(grads[k], held.at[k], loads.at[k, 1]),
            )
        )
        for fetch in fetches[k]:
            fetch.start()
    rows, width = right.shape[1:]
    chunk = chunk_of(rows)
    zero = jnp.zeros((8, width), jnp.float32)
    sums = (zero, zero)
    for k in range(6):
        for fetch in fetches[k]:
            fetch.wait()

        def piece(step, carry):
            span = pl.ds(pl.multiple_of(step * chunk, chunk), chunk)
            value, grad = right[k, span], held[k, span]
            return carry[0] + folded(value * grad), carry[1] + folded(grad * grad)

        sums = lax.fori_loop(0, rows // chunk, piece, sums)
    for k, value in enumerate((norm[...],) + sums):
        narrow = value[:, :128]
        for lane in range(128, width, 128):
            narrow = narrow + value[:, lane:lane + 128]
        packed[k] = narrow
    pl.semaphore_wait(barrier, total - 1)
    copies = [
        remote(packed, slots.at[me], send.at[step], receive.at[step], other(step))
        for step in range(1, total)
    ]
    slots[me] = packed[...]
    for copy in copies:
        copy.wait_recv()
    whole = jnp.sum(slots[...], axis=0)
    normed, crossed, squared = (jnp.sum(whole[k], axis=(0, 1), keepdims=True) for k in range(3))
    damp = damping[...]
    along = crossed * scale + damp * normed
    image = squared * (scale * scale) + 2.0 * damp * scale * crossed + damp * damp * normed
    alpha = normed / along
    after = normed - 2.0 * alpha * along + alpha * alpha * image
    beta = after / normed
    for k, value in enumerate((alpha, 1.0 + beta - alpha * damp, alpha * scale)):
        out[k:k + 1] = jnp.broadcast_to(value, (1, 128))
    for copy in copies:
        copy.wait_send()


def coefficients(dp, mp, scale, norm, damping, rhs, grads, ident):
    total = dp * mp
    hidden, width = rhs[0].shape[1:]
    dma = pltpu.SemaphoreType.DMA
    vmem, anywhere = pl.BlockSpec(memory_space=pltpu.VMEM), pl.BlockSpec(memory_space=pl.ANY)
    out = pl.pallas_call(
        functools.partial(scalar_kernel, dp, mp, scale),
        out_shape=jax.ShapeDtypeStruct((8, 128), jnp.float32),
        in_specs=[vmem, vmem] + [anywhere] * 9,
        out_specs=vmem,
        scratch_shapes=[
            pltpu.VMEM((6, hidden, width), jnp.float32),
            pltpu.VMEM((6, hidden, width), jnp.float32),
            pltpu.VMEM((3, 8, 128), jnp.float32),
            pltpu.VMEM((total, 3, 8, 128), jnp.float32),
            dma((6, 2)), dma((total,)), dma((total,)),
        ],
        compiler_params=pltpu.CompilerParams(
            collective_id=ident, has_side_effects=True, vmem_limit_bytes=32 * 1024 * 1024
        ),
    )(norm, damping.reshape(1, 1), *rhs, *grads)
    return out[0, 0], out[1, 0], out[2, 0]


def silu_terms(value):
    sigmoid_value = jax.nn.sigmoid(value)
    return (value * sigmoid_value, sigmoid_value * (1.0 + value * (1.0 - sigmoid_value)))


def matmul(left, right):
    return jnp.dot(left, right, preferred_element_type=jnp.float32)


def rows_product(left, right):
    return lax.dot_general(
        left, right, (((0,), (0,)), ((), ())), preferred_element_type=jnp.float32
    )


def against(left, right):
    return lax.dot_general(
        left, right, (((1,), (1,)), ((), ())), preferred_element_type=jnp.float32
    )


def body(tokens, gate_weights, up_weights, down_weights, rhs_gate, rhs_up, rhs_down, damping):
    dp, mp = lax.axis_size("dp"), lax.axis_size("mp")
    scale = 1.0 / (tokens.shape[0] * dp)
    turned = (rhs_gate.transpose(0, 2, 1), rhs_up.transpose(0, 2, 1), rhs_down)
    whole, norm, tangents = gathered(mp, tokens, turned, 0)
    tangent_gate, tangent_up, tangent_down, later_gate, later_up, later_down = tangents
    gate_one = matmul(whole, gate_weights[0])
    up_one = matmul(whole, up_weights[0])
    active_one, slope_one = silu_terms(gate_one)
    hidden_one = (active_one * up_one).astype(jnp.bfloat16)
    tan_gate = against(whole, tangent_gate)
    tan_up = against(whole, tangent_up)
    tan_hidden = (slope_one * up_one * tan_gate + active_one * tan_up).astype(jnp.bfloat16)
    layer_one, tan_layer = summed_whole(
        mp,
        (
            matmul(hidden_one, down_weights[0]),
            matmul(tan_hidden, down_weights[0]) + matmul(hidden_one, tangent_down),
        ),
        (whole, None),
        1,
    )
    gate_two = matmul(layer_one, gate_weights[1])
    up_two = matmul(layer_one, up_weights[1])
    active_two, slope_two = silu_terms(gate_two)
    hidden_two = (active_two * up_two).astype(jnp.bfloat16)
    tan_gate = matmul(tan_layer, gate_weights[1]) + against(layer_one, later_gate)
    tan_up = matmul(tan_layer, up_weights[1]) + against(layer_one, later_up)
    tan_hidden = (slope_two * up_two * tan_gate + active_two * tan_up).astype(jnp.bfloat16)
    (cotan,) = summed_whole(
        mp,
        (matmul(tan_hidden, down_weights[1]) + matmul(hidden_two, later_down),),
        (tan_layer,),
        2,
    )
    back_hidden = against(cotan, down_weights[1])
    back_gate = (back_hidden * up_two * slope_two).astype(jnp.bfloat16)
    back_up = (back_hidden * active_two).astype(jnp.bfloat16)
    back_layer, gates, ups, hiddens, first_hiddens, layers, cotans, inputs = summed_whole(
        mp,
        (against(back_gate, gate_weights[1]) + against(back_up, up_weights[1]),),
        (cotan,),
        3,
        (back_gate, back_up, hidden_two, hidden_one),
        (layer_one, cotan, whole),
    )
    second = (rows_product(gates, layers), rows_product(ups, layers), rows_product(hiddens, cotans))
    back_hidden = against(back_layer, down_weights[0])
    back_gate = (back_hidden * up_one * slope_one).astype(jnp.bfloat16)
    back_up = (back_hidden * active_one).astype(jnp.bfloat16)
    gates, ups, backs = swapped((back_gate, back_up), (back_layer,), 5)
    first = (rows_product(gates, inputs), rows_product(ups, inputs), rows_product(first_hiddens, backs))
    grads = (first, second)
    alpha, keep, drop = coefficients(dp, mp, scale, norm, damping, turned, first + second, 4)
    steps = [alpha * turned[k] for k in range(3)]
    nexts = [
        jnp.stack([keep * turned[k][layer] - drop * grads[layer][k] for layer in range(2)])
        for k in range(3)
    ]
    for arrays in (steps, nexts):
        arrays[0], arrays[1] = arrays[0].transpose(0, 2, 1), arrays[1].transpose(0, 2, 1)
    return tuple(steps) + tuple(nexts)


def solution(mesh):
    in_specs = (
        P("dp", "mp"),
        P(None, None, "mp"),
        P(None, None, "mp"),
        P(None, "mp", None),
        P(None, "dp", "mp"),
        P(None, "dp", "mp"),
        P(None, "mp", "dp"),
        P(),
    )
    out_specs = (
        P(None, "dp", "mp"),
        P(None, "dp", "mp"),
        P(None, "mp", "dp"),
        P(None, "dp", "mp"),
        P(None, "dp", "mp"),
        P(None, "mp", "dp"),
    )
    return jax.shard_map(body, mesh=mesh, in_specs=in_specs, out_specs=out_specs, check_vma=False)
```

```python
import functools
import jax
import jax.numpy as jnp
from jax import lax
from jax.experimental import pallas as pl
from jax.experimental.pallas import tpu as pltpu
from jax.sharding import PartitionSpec as P

LIMIT = 24 * 1024 * 1024
MESH = pl.DeviceIdType.MESH


def split_of(count):
    inner = 1
    while inner * inner < count and count % (inner * 2) == 0:
        inner *= 2
    return count // inner, inner


def greet(peers):
    barrier = pltpu.get_barrier_semaphore()
    for peer in peers:
        pl.semaphore_signal(barrier, inc=1, device_id=peer, device_id_type=MESH)
    pl.semaphore_wait(barrier, len(peers))


def place(outer, inner):
    me = lax.axis_index("mp")
    far, near = lax.div(me, inner), lax.rem(me, inner)

    def along_outer(step):
        return {"mp": lax.rem(far + step, outer) * inner + near}

    def along_inner(step):
        return {"mp": far * inner + lax.rem(near + step, inner)}

    return far, near, along_outer, along_inner


def remote(source, target, send, receive, peer):
    copy = pltpu.make_async_remote_copy(
        src_ref=source, dst_ref=target, send_sem=send, recv_sem=receive,
        device_id=peer, device_id_type=MESH,
    )
    copy.start()
    return copy


def start_pairs(sources, pairs, send, receive):
    row = lax.axis_index("dp")
    copies = []
    for k, (source, pair) in enumerate(zip(sources, pairs)):
        width = pair.shape[-1]
        if source.shape[-1] == width:
            outgoing = source
        else:
            outgoing = source.at[:, pl.ds(pl.multiple_of((1 - row) * width, width), width)]
        copies.append(remote(outgoing, pair.at[1], send.at[k], receive.at[k], {"dp": 1 - row}))
    return copies


def keep_pairs(sources, pairs):
    row = lax.axis_index("dp")
    for source, pair in zip(sources, pairs):
        width = pair.shape[-1]
        if source.shape[-1] == width:
            pair[0] = source[...]
        else:
            pair[0] = source[:, pl.ds(pl.multiple_of(row * width, width), width)]


def sum_kernel(outer, inner, count, adds, paired, *refs):
    parts = refs[:count]
    extra = dict(zip(adds, refs[count:count + len(adds)]))
    base = count + len(adds)
    sources = refs[base:base + paired]
    base += paired
    outs = refs[base:base + count]
    base += count
    pairs = refs[base:base + paired]
    base += paired
    lanes = lanes_of(outer, inner, parts[0].shape[-1], refs[base:])
    far, near, along_outer, along_inner = place(outer, inner)
    peers = [along_outer(e) for e in range(1, outer)] + [along_inner(d) for d in range(1, inner)]
    if paired:
        peers.append({"dp": 1 - lax.axis_index("dp")})
    greet(peers)
    sent = []

    def roles(lane):
        if lane["far_first"]:
            return far, near, along_outer, along_inner
        return near, far, along_inner, along_outer

    def spot(ref, lane, one, two):
        index = (two, one) if lane["far_first"] else (one, two)
        return ref.at[index[0], index[1], :, lane["columns"]]

    def launch(*call):
        copy = remote(*call)
        sent.append(copy)
        return copy

    first, second, third, fourth, own = {}, {}, {}, {}, {}
    for lane in lanes:
        one, two, along_one, along_two = roles(lane)
        for e in lane["order"]:
            piece = lax.rem(two + e, lane["twos"])
            for k in range(count):
                for d in range(1, lane["ones"]):
                    target = lax.rem(one + d, lane["ones"])
                    first[lane["name"], k, d, e] = launch(
                        spot(parts[k], lane, target, piece), lane["slots"].at[k, d, e],
                        lane["s1s"].at[k, d, e], lane["s1r"].at[k, d, e], along_one(d),
                    )
    swaps = start_pairs(sources, pairs, *refs[base + 22:]) if paired else []
    keep_pairs(sources, pairs)
    for turn in range(max(outer, inner)):
        for lane in lanes:
            if turn >= lane["twos"]:
                continue
            e = lane["order"][turn]
            one, two, along_one, along_two = roles(lane)
            piece = lax.rem(two + e, lane["twos"])
            for k in range(count):
                total = spot(parts[k], lane, one, piece)[...].astype(jnp.float32)
                for d in range(1, lane["ones"]):
                    first[lane["name"], k, d, e].wait_recv()
                    total = total + lane["slots"][k, d, e].astype(jnp.float32)
                if e:
                    lane["held"][k, e] = total.astype(jnp.bfloat16)
                    second[lane["name"], k, e] = launch(
                        lane["held"].at[k, e], lane["ends"].at[k, e],
                        lane["s2s"].at[k, e], lane["s2r"].at[k, e], along_two(e),
                    )
                else:
                    own[lane["name"], k] = total
    for lane in lanes:
        one, two, along_one, along_two = roles(lane)
        for k in range(count):
            total = own[lane["name"], k]
            for e in range(1, lane["twos"]):
                second[lane["name"], k, e].wait_recv()
                total = total + lane["ends"][k, e].astype(jnp.float32)
            if k in extra:
                total = total + spot(extra[k], lane, one, two)[...].astype(jnp.float32)
            block = spot(outs[k], lane, one, two)
            block[...] = total.astype(jnp.bfloat16)
            for e in range(1, lane["twos"]):
                third[lane["name"], k, e] = launch(
                    block, block, lane["g1s"].at[k, e], lane["g1r"].at[k, e], along_two(e)
                )
            for d in range(1, lane["ones"]):
                fourth[lane["name"], k, d, 0] = launch(
                    block, block, lane["g2s"].at[k, d, 0], lane["g2r"].at[k, d, 0], along_one(d)
                )
    for e in range(1, max(outer, inner)):
        for lane in lanes:
            if e >= lane["twos"]:
                continue
            one, two, along_one, along_two = roles(lane)
            piece = lax.rem(two - e + lane["twos"], lane["twos"])
            for k in range(count):
                third[lane["name"], k, e].wait_recv()
                block = spot(outs[k], lane, one, piece)
                for d in range(1, lane["ones"]):
                    fourth[lane["name"], k, d, e] = launch(
                        block, block, lane["g2s"].at[k, d, e], lane["g2r"].at[k, d, e], along_one(d)
                    )
    for copy in fourth.values():
        copy.wait_recv()
    for copy in swaps:
        copy.wait()
    for copy in sent:
        copy.wait_send()


def cut_of(width):
    return max(width * 13 // 16 // 128 * 128, 128)


def lane_scratch(count, ones, twos, share, width):
    dma = pltpu.SemaphoreType.DMA
    return [
        pltpu.VMEM((count, ones, twos, share, width), jnp.bfloat16),
        pltpu.VMEM((count, twos, share, width), jnp.bfloat16),
        pltpu.VMEM((count, twos, share, width), jnp.bfloat16),
        dma((count, ones, twos)), dma((count, ones, twos)),
        dma((count, twos)), dma((count, twos)),
        dma((count, twos)), dma((count, twos)),
        dma((count, ones, twos)), dma((count, ones, twos)),
    ]


def lanes_of(outer, inner, width, refs):
    cut = cut_of(width)
    names = ("slots", "held", "ends", "s1s", "s1r", "s2s", "s2r", "g1s", "g1r", "g2s", "g2r")
    lanes = []
    for far_first in (True, False):
        ones, twos = (outer, inner) if far_first else (inner, outer)
        lane = dict(zip(names, refs[11 * far_first:]))
        lane.update(
            name=int(far_first), far_first=far_first, ones=ones, twos=twos,
            order=list(range(1, twos)) + [0],
            columns=pl.ds(cut, width - cut) if far_first else pl.ds(0, cut),
        )
        lanes.append(lane)
    return lanes


def summed_whole(mp, parts, adds, ident, full=(), half=()):
    outer, inner = split_of(mp)
    rows, width = parts[0].shape
    share = rows // mp
    count = len(parts)
    view = (inner, outer, share, width)
    which = tuple(k for k in range(count) if adds[k] is not None)
    operands = [p.astype(jnp.bfloat16).reshape(view) for p in parts]
    operands += [adds[k].reshape(view) for k in which]
    dma = pltpu.SemaphoreType.DMA
    paired = len(full) + len(half)
    operands += list(full) + list(half)
    outs = pl.pallas_call(
        functools.partial(sum_kernel, outer, inner, count, which, paired),
        out_shape=[pltpu.VMEM(view, jnp.bfloat16)] * count + pair_shapes(full, half),
        in_specs=[pl.BlockSpec(memory_space=pltpu.VMEM)] * len(operands),
        out_specs=[pl.BlockSpec(memory_space=pltpu.VMEM)] * (count + paired),
        scratch_shapes=lane_scratch(count, inner, outer, share, cut_of(width))
        + lane_scratch(count, outer, inner, share, width - cut_of(width))
        + [dma((paired,))] * (2 if paired else 0),
        compiler_params=pltpu.CompilerParams(
            collective_id=ident, has_side_effects=True, vmem_limit_bytes=LIMIT
        ),
    )(*operands)
    return [o.reshape(rows, width) for o in outs[:count]] + joined(outs[count:])


def pair_shapes(full, half):
    return [jax.ShapeDtypeStruct((2,) + x.shape, x.dtype) for x in full] + [
        jax.ShapeDtypeStruct((2, x.shape[0], x.shape[1] // 2), x.dtype) for x in half
    ]


def joined(pairs):
    return [p.reshape(2 * p.shape[1], p.shape[2]) for p in pairs]


def pair_kernel(paired, *refs):
    sources, pairs = refs[:paired], refs[paired:2 * paired]
    greet([{"dp": 1 - lax.axis_index("dp")}])
    copies = start_pairs(sources, pairs, *refs[2 * paired:])
    keep_pairs(sources, pairs)
    for copy in copies:
        copy.wait()


def swapped(full, half, ident):
    paired = len(full) + len(half)
    spec = [pl.BlockSpec(memory_space=pltpu.VMEM)] * paired
    dma = pltpu.SemaphoreType.DMA
    return joined(
        pl.pallas_call(
            functools.partial(pair_kernel, paired),
            out_shape=pair_shapes(full, half),
            in_specs=spec,
            out_specs=spec,
            scratch_shapes=[dma((paired,)), dma((paired,))],
            compiler_params=pltpu.CompilerParams(
                collective_id=ident, has_side_effects=True, vmem_limit_bytes=LIMIT // 2
            ),
        )(*full, *half)
    )


def chunk_of(rows):
    return next(c for c in (64, 112, 32, 16, 8) if rows % c == 0)


def folded(block):
    return jnp.sum(block.reshape(block.shape[0] // 8, 8, block.shape[1]), axis=0)


def gather_kernel(outer, inner, mine, gate, up, down, out, norm, *refs):
    tangents, scratch = refs[:6], refs[6:]
    held, local, loads, g1s, g1r, g2s, g2r, ts, tr = scratch
    blocks = [(source, layer) for layer in range(2) for source in (gate, up, down)]
    fetches = []
    for k, (source, layer) in enumerate(blocks):
        fetches.append(pltpu.make_async_copy(source.at[layer], held.at[k], loads.at[k]))
        fetches[k].start()
    far, near, along_outer, along_inner = place(outer, inner)
    row = lax.axis_index("dp")
    greet(
        [along_outer(e) for e in range(1, outer)]
        + [along_inner(d) for d in range(1, inner)]
        + [{"dp": 1 - row}]
    )
    third, fourth = {}, {}
    keep = pltpu.make_async_copy(mine, out.at[far, near], local)
    keep.start()
    for e in range(1, outer):
        third[e] = remote(mine, out.at[far, near], g1s.at[e], g1r.at[e], along_outer(e))
    for d in range(1, inner):
        fourth[d, 0] = remote(mine, out.at[far, near], g2s.at[d, 0], g2r.at[d, 0], along_inner(d))
    rows, width = held.shape[1:]
    chunk = chunk_of(rows)
    columns = pl.ds(pl.multiple_of(row * width, width), width)
    total = jnp.zeros((8, width), jnp.float32)
    swaps = []

    def convert(k, total):
        fetches[k].wait()

        def piece(step, carry):
            span = pl.ds(pl.multiple_of(step * chunk, chunk), chunk)
            value = held[k, span]
            tangents[k][span, columns] = value.astype(jnp.bfloat16)
            return carry + folded(value * value)

        total = lax.fori_loop(0, rows // chunk, piece, total)
        swaps.append(
            remote(tangents[k].at[:, columns], tangents[k].at[:, columns], ts.at[k], tr.at[k], {"dp": 1 - row})
        )
        return total

    def relay(e):
        piece = lax.rem(far - e + outer, outer)
        third[e].wait_recv()
        for d in range(1, inner):
            fourth[d, e] = remote(
                out.at[piece, near], out.at[piece, near], g2s.at[d, e], g2r.at[d, e], along_inner(d)
            )

    total = convert(0, total)
    total = convert(1, total)
    for e in range(1, outer):
        relay(e)
    for k in range(2, 6):
        total = convert(k, total)
    norm[...] = total
    for copy in fourth.values():
        copy.wait_recv()
    keep.wait()
    for copy in swaps:
        copy.wait()
    for table in (third, fourth):
        for copy in table.values():
            copy.wait_send()


def gathered(mp, tokens, rhs, ident):
    outer, inner = split_of(mp)
    rows, share = tokens.shape
    hidden, width = rhs[0].shape[1:]
    dma = pltpu.SemaphoreType.DMA
    vmem, anywhere = pl.BlockSpec(memory_space=pltpu.VMEM), pl.BlockSpec(memory_space=pl.ANY)
    out, norm, *tangents = pl.pallas_call(
        functools.partial(gather_kernel, outer, inner),
        out_shape=[
            jax.ShapeDtypeStruct((outer, inner, rows, share), tokens.dtype),
            jax.ShapeDtypeStruct((8, width), jnp.float32),
        ] + [jax.ShapeDtypeStruct((hidden, 2 * width), jnp.bfloat16)] * 6,
        in_specs=[vmem] + [anywhere] * 3,
        out_specs=[vmem] * 8,
        scratch_shapes=[
            pltpu.VMEM((6, hidden, width), jnp.float32),
            dma, dma((6,)), dma((outer,)), dma((outer,)), dma((inner, outer)), dma((inner, outer)),
            dma((6,)), dma((6,)),
        ],
        compiler_params=pltpu.CompilerParams(
            collective_id=ident, has_side_effects=True, vmem_limit_bytes=48 * 1024 * 1024
        ),
    )(tokens, *rhs)
    whole = out.reshape(mp, rows, share).transpose(1, 0, 2).reshape(rows, mp * share)
    return whole, norm, tangents


def scalar_kernel(dp, mp, scale, norm, damping, gate, up, down, *refs):
    grads, out, rights, helds = refs[:6], refs[6], refs[7:10], refs[10:13]
    packed, slots, loads, send, receive = refs[13:]
    row, column = lax.axis_index("dp"), lax.axis_index("mp")
    total = dp * mp
    me = row * mp + column

    def other(step):
        index = lax.rem(me + step, total)
        return {"dp": lax.div(index, mp), "mp": lax.rem(index, mp)}

    barrier = pltpu.get_barrier_semaphore()
    for step in range(1, total):
        pl.semaphore_signal(barrier, inc=1, device_id=other(step), device_id_type=MESH)
    blocks = [(source, layer) for layer in range(2) for source in (gate, up, down)]
    fetches = []
    for k, (source, layer) in enumerate(blocks):
        fetches.append(
            (
                pltpu.make_async_copy(source.at[layer], rights[k % 3].at[layer], loads.at[k, 0]),
                pltpu.make_async_copy(grads[k], helds[k % 3].at[layer], loads.at[k, 1]),
            )
        )
        for fetch in fetches[k]:
            fetch.start()
    rows, width = rights[0].shape[1:]
    chunk = chunk_of(rows)
    zero = jnp.zeros((8, width), jnp.float32)
    sums = (zero, zero)
    for k in range(6):
        for fetch in fetches[k]:
            fetch.wait()

        def piece(step, carry):
            span = pl.ds(pl.multiple_of(step * chunk, chunk), chunk)
            value, grad = rights[k % 3][k // 3, span], helds[k % 3][k // 3, span]
            return carry[0] + folded(value * grad), carry[1] + folded(grad * grad)

        sums = lax.fori_loop(0, rows // chunk, piece, sums)
    for k, value in enumerate((norm[...],) + sums):
        narrow = value[:, :128]
        for lane in range(128, width, 128):
            narrow = narrow + value[:, lane:lane + 128]
        packed[k] = narrow
    pl.semaphore_wait(barrier, total - 1)
    copies = [
        remote(packed, slots.at[me], send.at[step], receive.at[step], other(step))
        for step in range(1, total)
    ]
    slots[me] = packed[...]
    for copy in copies:
        copy.wait_recv()
    whole = jnp.sum(slots[...], axis=0)
    normed, crossed, squared = (jnp.sum(whole[k], axis=(0, 1), keepdims=True) for k in range(3))
    damp = damping[...]
    along = crossed * scale + damp * normed
    image = squared * (scale * scale) + 2.0 * damp * scale * crossed + damp * damp * normed
    alpha = normed / along
    after = normed - 2.0 * alpha * along + alpha * alpha * image
    beta = after / normed
    for k, value in enumerate((alpha, 1.0 + beta - alpha * damp, alpha * scale)):
        out[k:k + 1] = jnp.broadcast_to(value, (1, 128))
    for copy in copies:
        copy.wait_send()


def coefficients(dp, mp, scale, norm, damping, rhs, grads, ident):
    total = dp * mp
    hidden, width = rhs[0].shape[1:]
    dma = pltpu.SemaphoreType.DMA
    vmem, anywhere = pl.BlockSpec(memory_space=pltpu.VMEM), pl.BlockSpec(memory_space=pl.ANY)
    out, *kept = pl.pallas_call(
        functools.partial(scalar_kernel, dp, mp, scale),
        out_shape=[jax.ShapeDtypeStruct((8, 128), jnp.float32)]
        + [pltpu.VMEM((2, hidden, width), jnp.float32)] * 6,
        in_specs=[vmem, vmem] + [anywhere] * 9,
        out_specs=[vmem] * 7,
        scratch_shapes=[
            pltpu.VMEM((3, 8, 128), jnp.float32),
            pltpu.VMEM((total, 3, 8, 128), jnp.float32),
            dma((6, 2)), dma((total,)), dma((total,)),
        ],
        compiler_params=pltpu.CompilerParams(
            collective_id=ident, has_side_effects=True, vmem_limit_bytes=32 * 1024 * 1024
        ),
    )(norm, damping.reshape(1, 1), *rhs, *grads)
    return out, kept[:3], kept[3:]


def finish_kernel(factors, *refs):
    rights, helds, outs, sems = refs[:3], refs[3:6], refs[6:12], refs[12:]
    steps, nexts, sem = sems
    alpha, keep, drop = (factors[k:k + 1, :1] for k in range(3))
    rows, width = rights[0].shape[1:]
    chunk = chunk_of(rows)
    copies = []
    for k in range(6):
        which, layer = k % 3, k // 3

        def piece(step, carry):
            span = pl.ds(pl.multiple_of(step * chunk, chunk), chunk)
            value = rights[which][layer, span]
            steps[k, span] = alpha * value
            nexts[k, span] = keep * value - drop * helds[which][layer, span]
            return carry

        lax.fori_loop(0, rows // chunk, piece, 0)
        for place_of, (source, target) in enumerate(
            ((steps, outs[which]), (nexts, outs[3 + which]))
        ):
            copy = pltpu.make_async_copy(source.at[k], target.at[layer], sem.at[k, place_of])
            copy.start()
            copies.append(copy)
    for copy in copies:
        copy.wait()


def finished(factors, rights, helds):
    shape = rights[0].shape
    vmem, anywhere = pl.BlockSpec(memory_space=pltpu.VMEM), pl.BlockSpec(memory_space=pl.ANY)
    return pl.pallas_call(
        finish_kernel,
        out_shape=[pltpu.HBM(shape, jnp.float32)] * 6,
        in_specs=[vmem] * 7,
        out_specs=[anywhere] * 6,
        scratch_shapes=[
            pltpu.VMEM((6,) + shape[1:], jnp.float32),
            pltpu.VMEM((6,) + shape[1:], jnp.float32),
            pltpu.SemaphoreType.DMA((6, 2)),
        ],
        compiler_params=pltpu.CompilerParams(vmem_limit_bytes=26 * 1024 * 1024),
    )(factors, *rights, *helds)


def silu_terms(value):
    sigmoid_value = jax.nn.sigmoid(value)
    return (value * sigmoid_value, sigmoid_value * (1.0 + value * (1.0 - sigmoid_value)))


def matmul(left, right):
    return jnp.dot(left, right, preferred_element_type=jnp.float32)


def rows_product(left, right):
    return lax.dot_general(
        left, right, (((0,), (0,)), ((), ())), preferred_element_type=jnp.float32
    )


def against(left, right):
    return lax.dot_general(
        left, right, (((1,), (1,)), ((), ())), preferred_element_type=jnp.float32
    )


def body(tokens, gate_weights, up_weights, down_weights, rhs_gate, rhs_up, rhs_down, damping):
    dp, mp = lax.axis_size("dp"), lax.axis_size("mp")
    scale = 1.0 / (tokens.shape[0] * dp)
    turned = (rhs_gate.transpose(0, 2, 1), rhs_up.transpose(0, 2, 1), rhs_down)
    whole, norm, tangents = gathered(mp, tokens, turned, 0)
    tangent_gate, tangent_up, tangent_down, later_gate, later_up, later_down = tangents
    gate_one = matmul(whole, gate_weights[0])
    up_one = matmul(whole, up_weights[0])
    active_one, slope_one = silu_terms(gate_one)
    hidden_one = (active_one * up_one).astype(jnp.bfloat16)
    tan_gate = against(whole, tangent_gate)
    tan_up = against(whole, tangent_up)
    tan_hidden = (slope_one * up_one * tan_gate + active_one * tan_up).astype(jnp.bfloat16)
    layer_one, tan_layer = summed_whole(
        mp,
        (
            matmul(hidden_one, down_weights[0]),
            matmul(tan_hidden, down_weights[0]) + matmul(hidden_one, tangent_down),
        ),
        (whole, None),
        1,
    )
    gate_two = matmul(layer_one, gate_weights[1])
    up_two = matmul(layer_one, up_weights[1])
    active_two, slope_two = silu_terms(gate_two)
    hidden_two = (active_two * up_two).astype(jnp.bfloat16)
    tan_gate = matmul(tan_layer, gate_weights[1]) + against(layer_one, later_gate)
    tan_up = matmul(tan_layer, up_weights[1]) + against(layer_one, later_up)
    tan_hidden = (slope_two * up_two * tan_gate + active_two * tan_up).astype(jnp.bfloat16)
    (cotan,) = summed_whole(
        mp,
        (matmul(tan_hidden, down_weights[1]) + matmul(hidden_two, later_down),),
        (tan_layer,),
        2,
    )
    back_hidden = against(cotan, down_weights[1])
    back_gate = (back_hidden * up_two * slope_two).astype(jnp.bfloat16)
    back_up = (back_hidden * active_two).astype(jnp.bfloat16)
    back_layer, gates, ups, hiddens, first_hiddens, layers, cotans, inputs = summed_whole(
        mp,
        (against(back_gate, gate_weights[1]) + against(back_up, up_weights[1]),),
        (cotan,),
        3,
        (back_gate, back_up, hidden_two, hidden_one),
        (layer_one, cotan, whole),
    )
    second = (rows_product(gates, layers), rows_product(ups, layers), rows_product(hiddens, cotans))
    back_hidden = against(back_layer, down_weights[0])
    back_gate = (back_hidden * up_one * slope_one).astype(jnp.bfloat16)
    back_up = (back_hidden * active_one).astype(jnp.bfloat16)
    gates, ups, backs = swapped((back_gate, back_up), (back_layer,), 5)
    first = (rows_product(gates, inputs), rows_product(ups, inputs), rows_product(first_hiddens, backs))
    factors, rights, helds = coefficients(
        dp, mp, scale, norm, damping, turned, first + second, 4
    )
    outs = finished(factors, rights, helds)
    steps, nexts = list(outs[:3]), list(outs[3:])
    for arrays in (steps, nexts):
        arrays[0], arrays[1] = arrays[0].transpose(0, 2, 1), arrays[1].transpose(0, 2, 1)
    return tuple(steps) + tuple(nexts)


def solution(mesh):
    in_specs = (
        P("dp", "mp"),
        P(None, None, "mp"),
        P(None, None, "mp"),
        P(None, "mp", None),
        P(None, "dp", "mp"),
        P(None, "dp", "mp"),
        P(None, "mp", "dp"),
        P(),
    )
    out_specs = (
        P(None, "dp", "mp"),
        P(None, "dp", "mp"),
        P(None, "mp", "dp"),
        P(None, "dp", "mp"),
        P(None, "dp", "mp"),
        P(None, "mp", "dp"),
    )
    return jax.shard_map(body, mesh=mesh, in_specs=in_specs, out_specs=out_specs, check_vma=False)
```

```python
import functools
import jax
import jax.numpy as jnp
from jax import lax
from jax.experimental import pallas as pl
from jax.experimental.pallas import tpu as pltpu
from jax.sharding import PartitionSpec as P

LIMIT = 24 * 1024 * 1024
MESH = pl.DeviceIdType.MESH


def split_of(count):
    inner = 1
    while inner * inner < count and count % (inner * 2) == 0:
        inner *= 2
    return count // inner, inner


def greet(peers):
    barrier = pltpu.get_barrier_semaphore()
    for peer in peers:
        pl.semaphore_signal(barrier, inc=1, device_id=peer, device_id_type=MESH)
    pl.semaphore_wait(barrier, len(peers))


def place(outer, inner):
    me = lax.axis_index("mp")
    far, near = lax.div(me, inner), lax.rem(me, inner)

    def along_outer(step):
        return {"mp": lax.rem(far + step, outer) * inner + near}

    def along_inner(step):
        return {"mp": far * inner + lax.rem(near + step, inner)}

    return far, near, along_outer, along_inner


def remote(source, target, send, receive, peer):
    copy = pltpu.make_async_remote_copy(
        src_ref=source, dst_ref=target, send_sem=send, recv_sem=receive,
        device_id=peer, device_id_type=MESH,
    )
    copy.start()
    return copy


def start_pairs(sources, pairs, send, receive):
    row = lax.axis_index("dp")
    copies = []
    for k, (source, pair) in enumerate(zip(sources, pairs)):
        width = pair.shape[-1]
        if source.shape[-1] == width:
            outgoing = source
        else:
            outgoing = source.at[:, pl.ds(pl.multiple_of((1 - row) * width, width), width)]
        copies.append(remote(outgoing, pair.at[1], send.at[k], receive.at[k], {"dp": 1 - row}))
    return copies


def keep_pairs(sources, pairs):
    row = lax.axis_index("dp")
    for source, pair in zip(sources, pairs):
        width = pair.shape[-1]
        if source.shape[-1] == width:
            pair[0] = source[...]
        else:
            pair[0] = source[:, pl.ds(pl.multiple_of(row * width, width), width)]


def sum_kernel(outer, inner, count, adds, paired, *refs):
    parts = refs[:count]
    extra = dict(zip(adds, refs[count:count + len(adds)]))
    base = count + len(adds)
    sources = refs[base:base + paired]
    base += paired
    outs = refs[base:base + count]
    base += count
    pairs = refs[base:base + paired]
    base += paired
    lanes = lanes_of(outer, inner, parts[0].shape[-1], refs[base:])
    far, near, along_outer, along_inner = place(outer, inner)
    peers = [along_outer(e) for e in range(1, outer)] + [along_inner(d) for d in range(1, inner)]
    if paired:
        peers.append({"dp": 1 - lax.axis_index("dp")})
    greet(peers)
    sent = []

    def roles(lane):
        if lane["far_first"]:
            return far, near, along_outer, along_inner
        return near, far, along_inner, along_outer

    def spot(ref, lane, one, two):
        index = (two, one) if lane["far_first"] else (one, two)
        return ref.at[index[0], index[1], :, lane["columns"]]

    def launch(*call):
        copy = remote(*call)
        sent.append(copy)
        return copy

    first, second, third, fourth, own = {}, {}, {}, {}, {}
    for lane in lanes:
        one, two, along_one, along_two = roles(lane)
        for e in lane["order"]:
            piece = lax.rem(two + e, lane["twos"])
            for k in range(count):
                for d in range(1, lane["ones"]):
                    target = lax.rem(one + d, lane["ones"])
                    first[lane["name"], k, d, e] = launch(
                        spot(parts[k], lane, target, piece), lane["slots"].at[k, d, e],
                        lane["s1s"].at[k, d, e], lane["s1r"].at[k, d, e], along_one(d),
                    )
    swaps = start_pairs(sources, pairs, *refs[base + 22:]) if paired else []
    keep_pairs(sources, pairs)
    for turn in range(max(outer, inner)):
        for lane in lanes:
            if turn >= lane["twos"]:
                continue
            e = lane["order"][turn]
            one, two, along_one, along_two = roles(lane)
            piece = lax.rem(two + e, lane["twos"])
            for k in range(count):
                total = spot(parts[k], lane, one, piece)[...].astype(jnp.float32)
                for d in range(1, lane["ones"]):
                    first[lane["name"], k, d, e].wait_recv()
                    total = total + lane["slots"][k, d, e].astype(jnp.float32)
                if e:
                    lane["held"][k, e] = total.astype(jnp.bfloat16)
                    second[lane["name"], k, e] = launch(
                        lane["held"].at[k, e], lane["ends"].at[k, e],
                        lane["s2s"].at[k, e], lane["s2r"].at[k, e], along_two(e),
                    )
                else:
                    own[lane["name"], k] = total
    for lane in lanes:
        one, two, along_one, along_two = roles(lane)
        for k in range(count):
            total = own[lane["name"], k]
            for e in range(1, lane["twos"]):
                second[lane["name"], k, e].wait_recv()
                total = total + lane["ends"][k, e].astype(jnp.float32)
            if k in extra:
                total = total + spot(extra[k], lane, one, two)[...].astype(jnp.float32)
            block = spot(outs[k], lane, one, two)
            block[...] = total.astype(jnp.bfloat16)
            for e in range(1, lane["twos"]):
                third[lane["name"], k, e] = launch(
                    block, block, lane["g1s"].at[k, e], lane["g1r"].at[k, e], along_two(e)
                )
            for d in range(1, lane["ones"]):
                fourth[lane["name"], k, d, 0] = launch(
                    block, block, lane["g2s"].at[k, d, 0], lane["g2r"].at[k, d, 0], along_one(d)
                )
    for e in range(1, max(outer, inner)):
        for lane in lanes:
            if e >= lane["twos"]:
                continue
            one, two, along_one, along_two = roles(lane)
            piece = lax.rem(two - e + lane["twos"], lane["twos"])
            for k in range(count):
                third[lane["name"], k, e].wait_recv()
                block = spot(outs[k], lane, one, piece)
                for d in range(1, lane["ones"]):
                    fourth[lane["name"], k, d, e] = launch(
                        block, block, lane["g2s"].at[k, d, e], lane["g2r"].at[k, d, e], along_one(d)
                    )
    for copy in fourth.values():
        copy.wait_recv()
    for copy in swaps:
        copy.wait()
    for copy in sent:
        copy.wait_send()


def cut_of(width):
    return max(width * 13 // 16 // 128 * 128, 128)


def lane_scratch(count, ones, twos, share, width):
    dma = pltpu.SemaphoreType.DMA
    return [
        pltpu.VMEM((count, ones, twos, share, width), jnp.bfloat16),
        pltpu.VMEM((count, twos, share, width), jnp.bfloat16),
        pltpu.VMEM((count, twos, share, width), jnp.bfloat16),
        dma((count, ones, twos)), dma((count, ones, twos)),
        dma((count, twos)), dma((count, twos)),
        dma((count, twos)), dma((count, twos)),
        dma((count, ones, twos)), dma((count, ones, twos)),
    ]


def lanes_of(outer, inner, width, refs):
    cut = cut_of(width)
    names = ("slots", "held", "ends", "s1s", "s1r", "s2s", "s2r", "g1s", "g1r", "g2s", "g2r")
    lanes = []
    for far_first in (True, False):
        ones, twos = (outer, inner) if far_first else (inner, outer)
        lane = dict(zip(names, refs[11 * far_first:]))
        lane.update(
            name=int(far_first), far_first=far_first, ones=ones, twos=twos,
            order=list(range(1, twos)) + [0],
            columns=pl.ds(cut, width - cut) if far_first else pl.ds(0, cut),
        )
        lanes.append(lane)
    return lanes


def summed_whole(mp, parts, adds, ident, full=(), half=()):
    outer, inner = split_of(mp)
    rows, width = parts[0].shape
    share = rows // mp
    count = len(parts)
    view = (inner, outer, share, width)
    which = tuple(k for k in range(count) if adds[k] is not None)
    operands = [p.astype(jnp.bfloat16).reshape(view) for p in parts]
    operands += [adds[k].reshape(view) for k in which]
    dma = pltpu.SemaphoreType.DMA
    paired = len(full) + len(half)
    operands += list(full) + list(half)
    outs = pl.pallas_call(
        functools.partial(sum_kernel, outer, inner, count, which, paired),
        out_shape=[pltpu.VMEM(view, jnp.bfloat16)] * count + pair_shapes(full, half),
        in_specs=[pl.BlockSpec(memory_space=pltpu.VMEM)] * len(operands),
        out_specs=[pl.BlockSpec(memory_space=pltpu.VMEM)] * (count + paired),
        scratch_shapes=lane_scratch(count, inner, outer, share, cut_of(width))
        + lane_scratch(count, outer, inner, share, width - cut_of(width))
        + [dma((paired,))] * (2 if paired else 0),
        compiler_params=pltpu.CompilerParams(
            collective_id=ident, has_side_effects=True, vmem_limit_bytes=LIMIT
        ),
    )(*operands)
    return [o.reshape(rows, width) for o in outs[:count]] + joined(outs[count:])


def pair_shapes(full, half):
    return [jax.ShapeDtypeStruct((2,) + x.shape, x.dtype) for x in full] + [
        jax.ShapeDtypeStruct((2, x.shape[0], x.shape[1] // 2), x.dtype) for x in half
    ]


def joined(pairs):
    return [p.reshape(2 * p.shape[1], p.shape[2]) for p in pairs]


def pair_kernel(paired, *refs):
    sources, pairs = refs[:paired], refs[paired:2 * paired]
    greet([{"dp": 1 - lax.axis_index("dp")}])
    copies = start_pairs(sources, pairs, *refs[2 * paired:])
    keep_pairs(sources, pairs)
    for copy in copies:
        copy.wait()


def swapped(full, half, ident):
    paired = len(full) + len(half)
    spec = [pl.BlockSpec(memory_space=pltpu.VMEM)] * paired
    dma = pltpu.SemaphoreType.DMA
    return joined(
        pl.pallas_call(
            functools.partial(pair_kernel, paired),
            out_shape=pair_shapes(full, half),
            in_specs=spec,
            out_specs=spec,
            scratch_shapes=[dma((paired,)), dma((paired,))],
            compiler_params=pltpu.CompilerParams(
                collective_id=ident, has_side_effects=True, vmem_limit_bytes=LIMIT // 2
            ),
        )(*full, *half)
    )


def chunk_of(rows):
    return next(c for c in (64, 112, 32, 16, 8) if rows % c == 0)


def folded(block):
    return jnp.sum(block.reshape(block.shape[0] // 8, 8, block.shape[1]), axis=0)


def gather_kernel(outer, inner, mine, gate, up, down, out, norm, *refs):
    tangents, scratch = refs[:6], refs[6:]
    held, local, loads, g1s, g1r, g2s, g2r, ts, tr = scratch
    blocks = [(source, layer) for layer in range(2) for source in (gate, up, down)]
    fetches = []
    for k, (source, layer) in enumerate(blocks):
        fetches.append(pltpu.make_async_copy(source.at[layer], held.at[k], loads.at[k]))
        fetches[k].start()
    far, near, along_outer, along_inner = place(outer, inner)
    row = lax.axis_index("dp")
    greet(
        [along_outer(e) for e in range(1, outer)]
        + [along_inner(d) for d in range(1, inner)]
        + [{"dp": 1 - row}]
    )
    third, fourth = {}, {}
    keep = pltpu.make_async_copy(mine, out.at[far, near], local)
    keep.start()
    for e in range(1, outer):
        third[e] = remote(mine, out.at[far, near], g1s.at[e], g1r.at[e], along_outer(e))
    for d in range(1, inner):
        fourth[d, 0] = remote(mine, out.at[far, near], g2s.at[d, 0], g2r.at[d, 0], along_inner(d))
    rows, width = held.shape[1:]
    chunk = chunk_of(rows)
    columns = pl.ds(pl.multiple_of(row * width, width), width)
    total = jnp.zeros((8, width), jnp.float32)
    swaps = []

    def convert(k, total):
        fetches[k].wait()

        def piece(step, carry):
            span = pl.ds(pl.multiple_of(step * chunk, chunk), chunk)
            value = held[k, span]
            tangents[k][span, columns] = value.astype(jnp.bfloat16)
            return carry + folded(value * value)

        total = lax.fori_loop(0, rows // chunk, piece, total)
        swaps.append(
            remote(tangents[k].at[:, columns], tangents[k].at[:, columns], ts.at[k], tr.at[k], {"dp": 1 - row})
        )
        return total

    def relay(e):
        piece = lax.rem(far - e + outer, outer)
        third[e].wait_recv()
        for d in range(1, inner):
            fourth[d, e] = remote(
                out.at[piece, near], out.at[piece, near], g2s.at[d, e], g2r.at[d, e], along_inner(d)
            )

    total = convert(0, total)
    total = convert(1, total)
    for e in range(1, outer):
        relay(e)
    for k in range(2, 6):
        total = convert(k, total)
    norm[...] = total
    for copy in fourth.values():
        copy.wait_recv()
    keep.wait()
    for copy in swaps:
        copy.wait()
    for table in (third, fourth):
        for copy in table.values():
            copy.wait_send()


def gathered(mp, tokens, rhs, ident):
    outer, inner = split_of(mp)
    rows, share = tokens.shape
    hidden, width = rhs[0].shape[1:]
    dma = pltpu.SemaphoreType.DMA
    vmem, anywhere = pl.BlockSpec(memory_space=pltpu.VMEM), pl.BlockSpec(memory_space=pl.ANY)
    out, norm, *tangents = pl.pallas_call(
        functools.partial(gather_kernel, outer, inner),
        out_shape=[
            jax.ShapeDtypeStruct((outer, inner, rows, share), tokens.dtype),
            jax.ShapeDtypeStruct((8, width), jnp.float32),
        ] + [jax.ShapeDtypeStruct((hidden, 2 * width), jnp.bfloat16)] * 6,
        in_specs=[vmem] + [anywhere] * 3,
        out_specs=[vmem] * 8,
        scratch_shapes=[
            pltpu.VMEM((6, hidden, width), jnp.float32),
            dma, dma((6,)), dma((outer,)), dma((outer,)), dma((inner, outer)), dma((inner, outer)),
            dma((6,)), dma((6,)),
        ],
        compiler_params=pltpu.CompilerParams(
            collective_id=ident, has_side_effects=True, vmem_limit_bytes=48 * 1024 * 1024
        ),
    )(tokens, *rhs)
    whole = out.reshape(mp, rows, share).transpose(1, 0, 2).reshape(rows, mp * share)
    return whole, norm, tangents


def scalar_kernel(dp, mp, scale, norm, damping, gate, up, down, *refs):
    grads, out, rights, helds = refs[:6], refs[6], refs[7:10], refs[10:13]
    packed, slots, loads, send, receive = refs[13:]
    row, column = lax.axis_index("dp"), lax.axis_index("mp")
    total = dp * mp
    me = row * mp + column

    def other(step):
        index = lax.rem(me + step, total)
        return {"dp": lax.div(index, mp), "mp": lax.rem(index, mp)}

    barrier = pltpu.get_barrier_semaphore()
    for step in range(1, total):
        pl.semaphore_signal(barrier, inc=1, device_id=other(step), device_id_type=MESH)
    blocks = [(source, layer) for layer in range(2) for source in (gate, up, down)]
    fetches = []
    for k, (source, layer) in enumerate(blocks):
        fetches.append(
            (
                pltpu.make_async_copy(source.at[layer], rights[k % 3].at[layer], loads.at[k, 0]),
                pltpu.make_async_copy(grads[k], helds[k % 3].at[layer], loads.at[k, 1]),
            )
        )
        for fetch in fetches[k]:
            fetch.start()
    rows, width = rights[0].shape[1:]
    chunk = chunk_of(rows)
    zero = jnp.zeros((8, width), jnp.float32)
    sums = (zero, zero)
    for k in range(6):
        for fetch in fetches[k]:
            fetch.wait()

        def piece(step, carry):
            span = pl.ds(pl.multiple_of(step * chunk, chunk), chunk)
            value, grad = rights[k % 3][k // 3, span], helds[k % 3][k // 3, span].astype(jnp.float32)
            return carry[0] + folded(value * grad), carry[1] + folded(grad * grad)

        sums = lax.fori_loop(0, rows // chunk, piece, sums)
    for k, value in enumerate((norm[...],) + sums):
        narrow = value[:, :128]
        for lane in range(128, width, 128):
            narrow = narrow + value[:, lane:lane + 128]
        packed[k] = narrow
    pl.semaphore_wait(barrier, total - 1)
    copies = [
        remote(packed, slots.at[me], send.at[step], receive.at[step], other(step))
        for step in range(1, total)
    ]
    slots[me] = packed[...]
    for copy in copies:
        copy.wait_recv()
    whole = jnp.sum(slots[...], axis=0)
    normed, crossed, squared = (jnp.sum(whole[k], axis=(0, 1), keepdims=True) for k in range(3))
    damp = damping[...]
    along = crossed * scale + damp * normed
    image = squared * (scale * scale) + 2.0 * damp * scale * crossed + damp * damp * normed
    alpha = normed / along
    after = normed - 2.0 * alpha * along + alpha * alpha * image
    beta = after / normed
    for k, value in enumerate((alpha, 1.0 + beta - alpha * damp, alpha * scale)):
        out[k:k + 1] = jnp.broadcast_to(value, (1, 128))
    for copy in copies:
        copy.wait_send()


def coefficients(dp, mp, scale, norm, damping, rhs, grads, ident):
    total = dp * mp
    hidden, width = rhs[0].shape[1:]
    dma = pltpu.SemaphoreType.DMA
    vmem, anywhere = pl.BlockSpec(memory_space=pltpu.VMEM), pl.BlockSpec(memory_space=pl.ANY)
    out, *kept = pl.pallas_call(
        functools.partial(scalar_kernel, dp, mp, scale),
        out_shape=[jax.ShapeDtypeStruct((8, 128), jnp.float32)]
        + [pltpu.VMEM((2, hidden, width), jnp.float32)] * 3
        + [pltpu.VMEM((2, hidden, width), jnp.bfloat16)] * 3,
        in_specs=[vmem, vmem] + [anywhere] * 9,
        out_specs=[vmem] * 7,
        scratch_shapes=[
            pltpu.VMEM((3, 8, 128), jnp.float32),
            pltpu.VMEM((total, 3, 8, 128), jnp.float32),
            dma((6, 2)), dma((total,)), dma((total,)),
        ],
        compiler_params=pltpu.CompilerParams(
            collective_id=ident, has_side_effects=True, vmem_limit_bytes=32 * 1024 * 1024
        ),
    )(norm, damping.reshape(1, 1), *rhs, *grads)
    return out, kept[:3], kept[3:]


def finish_kernel(factors, *refs):
    rights, helds, outs, sems = refs[:3], refs[3:6], refs[6:12], refs[12:]
    steps, nexts, sem = sems
    alpha, keep, drop = (factors[k:k + 1, :1] for k in range(3))
    rows, width = rights[0].shape[1:]
    chunk = chunk_of(rows)
    copies = []
    for k in range(6):
        which, layer = k % 3, k // 3

        def piece(step, carry):
            span = pl.ds(pl.multiple_of(step * chunk, chunk), chunk)
            value = rights[which][layer, span]
            steps[k, span] = alpha * value
            nexts[k, span] = keep * value - drop * helds[which][layer, span].astype(jnp.float32)
            return carry

        lax.fori_loop(0, rows // chunk, piece, 0)
        for place_of, (source, target) in enumerate(
            ((steps, outs[which]), (nexts, outs[3 + which]))
        ):
            copy = pltpu.make_async_copy(source.at[k], target.at[layer], sem.at[k, place_of])
            copy.start()
            copies.append(copy)
    for copy in copies:
        copy.wait()


def finished(factors, rights, helds):
    shape = rights[0].shape
    vmem, anywhere = pl.BlockSpec(memory_space=pltpu.VMEM), pl.BlockSpec(memory_space=pl.ANY)
    return pl.pallas_call(
        finish_kernel,
        out_shape=[pltpu.HBM(shape, jnp.float32)] * 6,
        in_specs=[vmem] * 7,
        out_specs=[anywhere] * 6,
        scratch_shapes=[
            pltpu.VMEM((6,) + shape[1:], jnp.float32),
            pltpu.VMEM((6,) + shape[1:], jnp.float32),
            pltpu.SemaphoreType.DMA((6, 2)),
        ],
        compiler_params=pltpu.CompilerParams(vmem_limit_bytes=26 * 1024 * 1024),
    )(factors, *rights, *helds)


def silu_terms(value):
    sigmoid_value = jax.nn.sigmoid(value)
    return (value * sigmoid_value, sigmoid_value * (1.0 + value * (1.0 - sigmoid_value)))


def matmul(left, right):
    return jnp.dot(left, right, preferred_element_type=jnp.float32)


def rows_product(left, right):
    return lax.dot_general(
        left, right, (((0,), (0,)), ((), ())), preferred_element_type=jnp.float32
    )


def against(left, right):
    return lax.dot_general(
        left, right, (((1,), (1,)), ((), ())), preferred_element_type=jnp.float32
    )


def body(tokens, gate_weights, up_weights, down_weights, rhs_gate, rhs_up, rhs_down, damping):
    dp, mp = lax.axis_size("dp"), lax.axis_size("mp")
    scale = 1.0 / (tokens.shape[0] * dp)
    turned = (rhs_gate.transpose(0, 2, 1), rhs_up.transpose(0, 2, 1), rhs_down)
    whole, norm, tangents = gathered(mp, tokens, turned, 0)
    tangent_gate, tangent_up, tangent_down, later_gate, later_up, later_down = tangents
    gate_one = matmul(whole, gate_weights[0])
    up_one = matmul(whole, up_weights[0])
    active_one, slope_one = silu_terms(gate_one)
    hidden_one = (active_one * up_one).astype(jnp.bfloat16)
    tan_gate = against(whole, tangent_gate)
    tan_up = against(whole, tangent_up)
    tan_hidden = (slope_one * up_one * tan_gate + active_one * tan_up).astype(jnp.bfloat16)
    layer_one, tan_layer = summed_whole(
        mp,
        (
            matmul(hidden_one, down_weights[0]),
            matmul(tan_hidden, down_weights[0]) + matmul(hidden_one, tangent_down),
        ),
        (whole, None),
        1,
    )
    gate_two = matmul(layer_one, gate_weights[1])
    up_two = matmul(layer_one, up_weights[1])
    active_two, slope_two = silu_terms(gate_two)
    hidden_two = (active_two * up_two).astype(jnp.bfloat16)
    tan_gate = matmul(tan_layer, gate_weights[1]) + against(layer_one, later_gate)
    tan_up = matmul(tan_layer, up_weights[1]) + against(layer_one, later_up)
    tan_hidden = (slope_two * up_two * tan_gate + active_two * tan_up).astype(jnp.bfloat16)
    (cotan,) = summed_whole(
        mp,
        (matmul(tan_hidden, down_weights[1]) + matmul(hidden_two, later_down),),
        (tan_layer,),
        2,
    )
    back_hidden = against(cotan, down_weights[1])
    back_gate = (back_hidden * up_two * slope_two).astype(jnp.bfloat16)
    back_up = (back_hidden * active_two).astype(jnp.bfloat16)
    back_layer, gates, ups, hiddens, first_hiddens, layers, cotans, inputs = summed_whole(
        mp,
        (against(back_gate, gate_weights[1]) + against(back_up, up_weights[1]),),
        (cotan,),
        3,
        (back_gate, back_up, hidden_two, hidden_one),
        (layer_one, cotan, whole),
    )
    second = (rows_product(gates, layers), rows_product(ups, layers), rows_product(hiddens, cotans))
    back_hidden = against(back_layer, down_weights[0])
    back_gate = (back_hidden * up_one * slope_one).astype(jnp.bfloat16)
    back_up = (back_hidden * active_one).astype(jnp.bfloat16)
    gates, ups, backs = swapped((back_gate, back_up), (back_layer,), 5)
    first = (rows_product(gates, inputs), rows_product(ups, inputs), rows_product(first_hiddens, backs))
    factors, rights, helds = coefficients(
        dp, mp, scale, norm, damping, turned,
        [grad.astype(jnp.bfloat16) for grad in first + second], 4
    )
    outs = finished(factors, rights, helds)
    steps, nexts = list(outs[:3]), list(outs[3:])
    for arrays in (steps, nexts):
        arrays[0], arrays[1] = arrays[0].transpose(0, 2, 1), arrays[1].transpose(0, 2, 1)
    return tuple(steps) + tuple(nexts)


def solution(mesh):
    in_specs = (
        P("dp", "mp"),
        P(None, None, "mp"),
        P(None, None, "mp"),
        P(None, "mp", None),
        P(None, "dp", "mp"),
        P(None, "dp", "mp"),
        P(None, "mp", "dp"),
        P(),
    )
    out_specs = (
        P(None, "dp", "mp"),
        P(None, "dp", "mp"),
        P(None, "mp", "dp"),
        P(None, "dp", "mp"),
        P(None, "dp", "mp"),
        P(None, "mp", "dp"),
    )
    return jax.shard_map(body, mesh=mesh, in_specs=in_specs, out_specs=out_specs, check_vma=False)
```
